16 devices in a mesh: pod: 2 (over z), data: 8 (over y, x, core).
Axes of the slice: x: 2, y: 2, z: 2, core: 2. Of those that a mesh axis runs over, the one named last changes fastest.
Arguments:
- w_first: float32 [12, 768, 3072], replicated
- w_second: float32 [12, 3072, 768], replicated
- m_first: float32 [12, 768, 3072], replicated
- m_second: float32 [12, 3072, 768], replicated
- x_now: bfloat16 [8192, 768], P(('pod', 'data'))
- y_now: bfloat16 [8192, 768], P(('pod', 'data'))
- x_next: bfloat16 [8192, 768], P(('pod', 'data'))
- y_next: bfloat16 [8192, 768], P(('pod', 'data'))
Outputs:
- output 1: float32 [12, 768, 3072], replicated
- output 2: float32 [12, 3072, 768], replicated
- output 3: float32 [12, 768, 3072], replicated
- output 4: float32 [12, 3072, 768], replicated
- output 5: float32 [8192], P(('pod', 'data'))
- output 6: float32 [8192, 768], P(('pod', 'data'))
All inputs are finite; a program needn't handle non-finite values.
Results may differ from the reference program's by a relative error of at most 0.0108314.
Values are sent between devices in bfloat16 or wider.
A program may use at most 3.5 GiB of HBM per device.

```python
import jax
import jax.numpy as jnp
from jax import lax

D = 768
F = 3072
LAYERS = 12
TOK = 512
DEVICES = 16
BATCH = TOK * DEVICES
LEARN_RATE = 0.25 / LAYERS
MOMENTUM = 0.9
BRANCH_SCALE = (4.0 / max(LAYERS, 4)) ** 0.5


def draw_batch(key_list):
    noise_val = jax.random.normal(key_list[0], (DEVICES, TOK, D), jnp.float32)
    global_off = jax.random.normal(key_list[1], (1, 1, D), jnp.float32)
    device_off = jax.random.normal(key_list[2], (DEVICES, 1, D), jnp.float32)
    rows_val = 0.7 * noise_val + 0.5 * global_off + 0.5 * device_off
    return rows_val.reshape(BATCH, D).astype(jnp.bfloat16)


def setup_inputs(seed: int = 0) -> dict:
    key_list = jax.random.split(jax.random.key(seed), 16)
    w_first = jax.random.normal(key_list[0], (LAYERS, D, F), jnp.float32) * D ** -0.5
    w_second = jax.random.normal(key_list[1], (LAYERS, F, D), jnp.float32) * (F ** -0.5 * BRANCH_SCALE)
    m_first = jax.random.normal(key_list[2], (LAYERS, D, F), jnp.float32) * (0.3 * BRANCH_SCALE / D)
    m_second = jax.random.normal(key_list[3], (LAYERS, F, D), jnp.float32) * (0.7 / D)
    return {'w_first': w_first, 'w_second': w_second, 'm_first': m_first, 'm_second': m_second,
            'x_now': draw_batch(key_list[4:7]), 'y_now': draw_batch(key_list[7:10]),
            'x_next': draw_batch(key_list[10:13]), 'y_next': draw_batch(key_list[13:16])}


def layer_stack(hidden, w_first_low, w_second_low):
    def body(carry, weights):
        pre_act = jnp.dot(carry.astype(jnp.bfloat16), weights[0], preferred_element_type=jnp.float32)
        act_low = jax.nn.gelu(pre_act).astype(jnp.bfloat16)
        return carry + jnp.dot(act_low, weights[1], preferred_element_type=jnp.float32), carry
    return lax.scan(body, hidden, (w_first_low, w_second_low))


def local_grads(rows_in, rows_target, w_first_low, w_second_low):
    h_last, h_saved = layer_stack(rows_in.astype(jnp.float32), w_first_low, w_second_low)
    grad_h = (h_last - rows_target.astype(jnp.float32)) / (BATCH * D)

    def back(grad_carry, layer_item):
        h_in, wf_low, ws_low = layer_item
        h_low = h_in.astype(jnp.bfloat16)
        pre_act = jnp.dot(h_low, wf_low, preferred_element_type=jnp.float32)
        act_val, gelu_back = jax.vjp(jax.nn.gelu, pre_act)
        act_low = act_val.astype(jnp.bfloat16)
        grad_low = grad_carry.astype(jnp.bfloat16)
        g_second = jnp.dot(act_low.T, grad_low, preferred_element_type=jnp.float32)
        grad_act = jnp.dot(grad_low, ws_low.T, preferred_element_type=jnp.float32)
        grad_pre = gelu_back(grad_act)[0].astype(jnp.bfloat16)
        g_first = jnp.dot(h_low.T, grad_pre, preferred_element_type=jnp.float32)
        grad_next = grad_carry + jnp.dot(grad_pre, wf_low.T, preferred_element_type=jnp.float32)
        return grad_next, (g_first.astype(jnp.bfloat16), g_second.astype(jnp.bfloat16))

    return lax.scan(back, grad_h, (h_saved, w_first_low, w_second_low), reverse=True)[1]


def reference(w_first, w_second, m_first, m_second, x_now, y_now, x_next, y_next):
    w_first_low = w_first.astype(jnp.bfloat16)
    w_second_low = w_second.astype(jnp.bfloat16)

    def add_device(grad_acc, rows_pair):
        g_first, g_second = local_grads(rows_pair[0], rows_pair[1], w_first_low, w_second_low)
        return (grad_acc[0] + g_first.astype(jnp.float32), grad_acc[1] + g_second.astype(jnp.float32)), None

    zero_acc = (jnp.zeros(w_first.shape, jnp.float32), jnp.zeros(w_second.shape, jnp.float32))
    rows_now = (x_now.reshape(DEVICES, TOK, D), y_now.reshape(DEVICES, TOK, D))
    (grad_first, grad_second), _ = lax.scan(add_device, zero_acc, rows_now)
    m_first_new = MOMENTUM * m_first + grad_first
    m_second_new = MOMENTUM * m_second + grad_second
    w_first_new = w_first - LEARN_RATE * m_first_new
    w_second_new = w_second - LEARN_RATE * m_second_new
    new_first_low = w_first_new.astype(jnp.bfloat16)
    new_second_low = w_second_new.astype(jnp.bfloat16)

    def next_device(rows_pair):
        h_last = layer_stack(rows_pair[0].astype(jnp.float32), new_first_low, new_second_low)[0]
        resid_rows = h_last - rows_pair[1].astype(jnp.float32)
        return h_last, jnp.sum(resid_rows * resid_rows, axis=-1) / (2 * D)

    rows_next = (x_next.reshape(DEVICES, TOK, D), y_next.reshape(DEVICES, TOK, D))
    h_out, loss_out = lax.map(next_device, rows_next)
    return (w_first_new, w_second_new, m_first_new, m_second_new,
            loss_out.reshape(BATCH), h_out.reshape(BATCH, D))
```

```python
import functools

import jax
import jax.numpy as jnp
from jax import lax
from jax.experimental import pallas as pl
from jax.experimental.pallas import tpu as pltpu
from jax.sharding import PartitionSpec as P

LEARN_BASE = 0.25
MOMENTUM = 0.9
GELU_C = 0.7978845608028654
GELU_A = 0.044715
BF = jnp.bfloat16
F32 = jnp.float32
MESH_ID = pl.DeviceIdType.MESH
BLK = 768
HALF = BLK // 2
PART = HALF // 3
NACC = 4
NFULL = 6
CHUNK = 256
NN = (((1,), (0,)), ((), ()))
NT = (((1,), (1,)), ((), ()))


def dot(lhs, rhs, dims=NN):
    return lax.dot_general(lhs, rhs, dims, preferred_element_type=F32)


def gelu(a):
    return a * (0.5 * (1.0 + jnp.tanh(GELU_C * (a + GELU_A * (a * a * a)))))


def gelu_pair(a):
    sq = a * a
    t = jnp.tanh(GELU_C * (a + GELU_A * (sq * a)))
    cdf = 0.5 * (1.0 + t)
    slope = cdf + a * (0.5 * (1.0 - t * t)) * (GELU_C * (1.0 + (3.0 * GELU_A) * sq))
    return a * cdf, slope


def step_kernel(layers, per_layer, scale, learn_rate,
                w1, w2, m1, m2, x_now, y_now, x_next,
                g1, g2, hs, h_out,
                wbuf, mbuf, gst, gfull, acc, land0, land1, land2, land3,
                hl, hl_t, low, state, actq, wlow, rows_in,
                ld_sem, hs_sem, io_sem, st_sem, own_sem,
                x0_s, x0_r, rs_s, rs_r, ag_s, ag_r, x7_s, x7_r, out_sem):
    units = layers * per_layer
    pod = lax.axis_index('pod')
    data = lax.axis_index('data')
    core = lax.rem(data, 2)
    cx = lax.rem(data // 2, 2)
    cy = data // 4
    partner = (pod, data + 1 - 2 * core)
    along = {'x': (cx, (pod, data + 2 - 4 * cx)),
             'y': (cy, (pod, data + 4 - 8 * cy)),
             'z': (pod, (1 - pod, data))}
    orders = ('xyz', 'yzx', 'zxy')

    barrier = pltpu.get_barrier_semaphore()
    for dev in (partner, along['x'][1], along['y'][1], along['z'][1]):
        pl.semaphore_signal(barrier, inc=1, device_id=dev, device_id_type=MESH_ID)
    pl.semaphore_wait(barrier, 4)

    def block_of(ref, k, layer, f):
        off = pl.multiple_of(f * BLK, BLK)
        if k == 0:
            return ref.at[layer, :, pl.ds(off, BLK)]
        return ref.at[layer, pl.ds(off, BLK), :]

    def loads(layer, f, par, full):
        out = []
        for k in range(2):
            out.append(pltpu.make_async_copy(block_of((w1, w2)[k], k, layer, f), wbuf.at[k, par], ld_sem.at[par, k]))
            if full:
                out.append(pltpu.make_async_copy(block_of((m1, m2)[k], k, layer, f), mbuf.at[k, par], ld_sem.at[par, 2 + k]))
                out.append(pltpu.make_async_copy(block_of((g1, g2)[k], k, layer, f), gst.at[k, par], ld_sem.at[par, 4 + k]))
        return out

    def start_all(copies):
        for c in copies:
            c.start()

    def wait_all(copies):
        for c in copies:
            c.wait()

    def cast_weights(par, full):
        def body(r, _):
            rows = pl.ds(pl.multiple_of(r * 64, 64), 64)
            for k in range(2):
                w = wbuf[k, par, rows, :]
                if full:
                    mom = MOMENTUM * mbuf[k, par, rows, :] + gst[k, par, rows, :].astype(F32)
                    w = w - learn_rate * mom
                wlow[k, rows, :] = w.astype(BF)
            return 0
        lax.fori_loop(0, BLK // 64, body, 0)

    def col(j):
        return pl.ds(pl.multiple_of(j * CHUNK, CHUNK), CHUNK)

    def load_rows(src):
        copy = pltpu.make_async_copy(src, rows_in, io_sem.at[0])
        copy.start()
        copy.wait()

    def save_h(layer):
        return pltpu.make_async_copy(low, hs.at[layer], hs_sem.at[0])

    def fetch_h(layer):
        slot = lax.rem(layer, 2)
        return pltpu.make_async_copy(hs.at[layer], hl.at[slot], hs_sem.at[slot])

    def forward_unit(i, full):
        layer, f, par = i // per_layer, lax.rem(i, per_layer), lax.rem(i, 2)
        wait_all(loads(layer, f, par, full))

        @pl.when(i + 1 < units)
        def _():
            nxt = i + 1
            start_all(loads(nxt // per_layer, lax.rem(nxt, per_layer), lax.rem(nxt, 2), full))

        @pl.when(f == 0)
        def _():
            if not full:
                @pl.when(layer > 0)
                def _():
                    save_h(layer - 1).wait()
            low[...] = state[...].astype(BF)
            if not full:
                save_h(layer).start()

        cast_weights(par, full)

        def first(j, _):
            a = dot(low[...], wlow[0, :, col(j)])
            actq[:, col(j)] = gelu(a).astype(BF)
            return 0
        lax.fori_loop(0, BLK // CHUNK, first, 0)

        def second(j, _):
            state[:, col(j)] += dot(actq[...], wlow[1, :, col(j)])
            return 0
        lax.fori_loop(0, BLK // CHUNK, second, 0)

    def back_place(b):
        return layers - 1 - b // per_layer, lax.rem(b, per_layer), lax.rem(b, 2)

    def store_grads(b):
        layer, f, par = back_place(b)
        return [pltpu.make_async_copy(gst.at[k, par], block_of((g1, g2)[k], k, layer, f), st_sem.at[par, k])
                for k in range(2)]

    def backward_unit(b):
        layer, f, par = back_place(b)
        wait_all(loads(layer, f, par, False))

        @pl.when(b + 1 < units)
        def _():
            nl, nf, np_ = back_place(b + 1)
            start_all(loads(nl, nf, np_, False))

        slot = lax.rem(layer, 2)

        @pl.when(f == 0)
        def _():
            fetch_h(layer).wait()

            @pl.when(layer > 0)
            def _():
                fetch_h(layer - 1).start()
            low[...] = state[...].astype(BF)
            hl_t[...] = hl[slot].T

        cast_weights(par, False)

        @pl.when(b >= 2)
        def _():
            wait_all(store_grads(b - 2))

        def body(j, _):
            a = dot(hl[slot], wlow[0, :, col(j)])
            du = dot(low[...], wlow[1, col(j), :], NT)
            u, slope = gelu_pair(a)
            q = (slope * du).astype(BF)
            actq[:, col(j)] = q
            gst[1, par, col(j), :] = dot(u.astype(BF).T, low[...]).astype(BF)
            gst[0, par, :, col(j)] = dot(hl_t[...], q).astype(BF)
            return 0
        lax.fori_loop(0, BLK // CHUNK, body, 0)

        @pl.when(layer > 0)
        def _():
            def carry(j, _):
                state[:, col(j)] += dot(actq[...], wlow[0, col(j), :], NT)
                return 0
            lax.fori_loop(0, BLK // CHUNK, carry, 0)
        start_all(store_grads(b))

    back_ticks = units // 3
    early = back_ticks // per_layer

    def comm_place(c):
        s = c // per_layer
        layer = jnp.where(s == 0, layers - 1,
                          jnp.where(s < early, layers - 2 - s,
                                    jnp.where(s < layers - 1, s - early, layers - 2)))
        return layer, lax.rem(c, per_layer)

    def x0_copies(c):
        layer, f = comm_place(c)
        out = []
        par = lax.rem(c, 2)
        slot = lax.rem(c, NACC)
        for k in range(2):
            def rows_of(start):
                if k == 0:
                    return g1.at[layer, pl.ds(pl.multiple_of(start, HALF), HALF), pl.ds(pl.multiple_of(f * BLK, BLK), BLK)]
                return g2.at[layer, pl.ds(pl.multiple_of(f * BLK + start, HALF), HALF), :]
            out.append(pltpu.make_async_remote_copy(
                src_ref=rows_of((1 - core) * HALF), dst_ref=land0.at[par, k],
                send_sem=x0_s.at[par, k], recv_sem=x0_r.at[par, k],
                device_id=partner, device_id_type=MESH_ID))
            out.append(pltpu.make_async_copy(rows_of(core * HALF), acc.at[slot, k], own_sem.at[par, k]))
        return out

    def offsets(p):
        coords = [along[a][0] for a in orders[p]]
        keep1 = p * PART + coords[0] * (PART // 2)
        send1 = p * PART + (1 - coords[0]) * (PART // 2)
        keep2 = keep1 + coords[1] * (PART // 4)
        send2 = keep1 + (1 - coords[1]) * (PART // 4)
        keep3 = keep2 + coords[2] * (PART // 8)
        send3 = keep2 + (1 - coords[2]) * (PART // 8)
        return (keep1, keep2, keep3), (send1, send2, send3)

    places = [offsets(p) for p in range(3)]
    lands = (land1, land2, land3)
    sizes = (PART // 2, PART // 4, PART // 8)

    def rs_copies(c, j):
        par, slot = lax.rem(c, 2), lax.rem(c, NACC)
        n = sizes[j]
        return [pltpu.make_async_remote_copy(
            src_ref=acc.at[slot, :, pl.ds(pl.multiple_of(places[p][1][j], 16), n), :],
            dst_ref=lands[j].at[par, :, pl.ds(p * n, n), :],
            send_sem=rs_s.at[j, par, p], recv_sem=rs_r.at[j, par, p],
            device_id=along[orders[p][j]][1], device_id_type=MESH_ID) for p in range(3)]

    def ag_copies(c, j):
        par, slot = lax.rem(c, 2), lax.rem(c, NFULL)
        n = sizes[2 - j]
        out = []
        for p in range(3):
            rows = pl.ds(pl.multiple_of(core * HALF + places[p][0][2 - j], 16), n)
            out.append(pltpu.make_async_remote_copy(
                src_ref=gfull.at[slot, :, rows, :], dst_ref=gfull.at[slot, :, rows, :],
                send_sem=ag_s.at[j, par, p], recv_sem=ag_r.at[j, par, p],
                device_id=along[orders[p][2 - j]][1], device_id_type=MESH_ID))
        return out

    def x7_copies(c):
        par, slot = lax.rem(c, 2), lax.rem(c, NFULL)
        rows = pl.ds(pl.multiple_of(core * HALF, HALF), HALF)
        return [pltpu.make_async_remote_copy(
            src_ref=gfull.at[slot, :, rows, :], dst_ref=gfull.at[slot, :, rows, :],
            send_sem=x7_s.at[par], recv_sem=x7_r.at[par],
            device_id=partner, device_id_type=MESH_ID)]

    def out_copies(c):
        layer, f = comm_place(c)
        par, slot = lax.rem(c, 2), lax.rem(c, NFULL)
        return [pltpu.make_async_copy(gfull.at[slot, k], block_of((g1, g2)[k], k, layer, f), out_sem.at[par, k])
                for k in range(2)]

    def stage(c, s):
        @pl.when((c >= 0) & (c < units))
        def _():
            par, slot = lax.rem(c, 2), lax.rem(c, NACC)
            if s == 0:
                start_all(x0_copies(c))
            elif s == 1:
                wait_all(x0_copies(c))

                def body(r, _):
                    rows = pl.ds(pl.multiple_of(r * 64, 64), 64)
                    for k in range(2):
                        acc[slot, k, rows, :] = (acc[slot, k, rows, :].astype(F32)
                                                 + land0[par, k, rows, :].astype(F32)).astype(BF)
                    return 0
                lax.fori_loop(0, HALF // 64, body, 0)
                start_all(rs_copies(c, 0))
            elif s in (2, 3, 4):
                j = s - 2
                copies = rs_copies(c, j)
                n = sizes[j]
                full_slot = lax.rem(c, NFULL)
                for p in range(3):
                    copies[p].wait()
                    rows = pl.ds(pl.multiple_of(places[p][0][j], 16), n)
                    for k in range(2):
                        total = (acc[slot, k, rows, :].astype(F32)
                                 + lands[j][par, k, p * n:(p + 1) * n, :].astype(F32)).astype(BF)
                        if s < 4:
                            acc[slot, k, rows, :] = total
                        else:
                            own = pl.ds(pl.multiple_of(core * HALF + places[p][0][j], 16), n)
                            gfull[full_slot, k, own, :] = total
                start_all(rs_copies(c, j + 1) if s < 4 else ag_copies(c, 0))
            elif s in (5, 6):
                wait_all(ag_copies(c, s - 5))
                start_all(ag_copies(c, s - 4))
            elif s == 7:
                wait_all(ag_copies(c, 2))
                start_all(x7_copies(c))
            elif s == 8:
                wait_all(x7_copies(c))
                start_all(out_copies(c))
            else:
                wait_all(out_copies(c))

    start_all(loads(0, 0, 0, False))
    load_rows(x_now)
    state[...] = rows_in[...].astype(F32)

    def fwd_now(i, _):
        forward_unit(i, False)
        return 0
    lax.fori_loop(0, units, fwd_now, 0)
    save_h(layers - 1).wait()
    fetch_h(layers - 1).start()
    start_all(loads(layers - 1, 0, 0, False))
    load_rows(y_now)
    state[...] = (state[...] - rows_in[...].astype(F32)) * scale

    late = (layers - 1 - early) * per_layer
    first_tick = back_ticks + 10
    burst_tick = first_tick + late
    burst = (early - 1) * per_layer // 3
    last_tick = burst_tick + burst

    def tick(t, _):
        for s in (9, 8, 7, 6, 5):
            stage(t - s, s)

        def back(j, _):
            backward_unit(3 * t + j)
            return 0
        lax.fori_loop(0, jnp.where(t < back_ticks, 3, 0), back, 0)

        @pl.when(t == back_ticks)
        def _():
            wait_all(store_grads(units - 2))
            wait_all(store_grads(units - 1))

        @pl.when(t == first_tick - 1)
        def _():
            start_all(loads(0, 0, 0, True))
            load_rows(x_next)
            state[...] = rows_in[...].astype(F32)

        count = jnp.where(t < first_tick, 0, jnp.where(t < burst_tick, 1, jnp.where(t < last_tick, 3, 2 * per_layer)))
        begin = jnp.where(t < burst_tick, t - first_tick,
                          jnp.where(t < last_tick, late + 3 * (t - burst_tick), late + 3 * burst))

        def ahead(j, _):
            forward_unit(begin + j, True)
            return 0
        lax.fori_loop(0, count, ahead, 0)

        for s in (4, 3, 2, 1, 0):
            stage(t - s, s)
        return 0
    lax.fori_loop(0, last_tick + 1, tick, 0)

    copy = pltpu.make_async_copy(state, h_out, io_sem.at[0])
    copy.start()
    copy.wait()


def build_kernel(w_first, rows, batch_total, learn_rate):
    layers, width, hidden = w_first.shape
    per_layer = hidden // BLK
    any_spec = pl.BlockSpec(memory_space=pl.ANY)
    dma = pltpu.SemaphoreType.DMA
    return pl.pallas_call(
        functools.partial(step_kernel, layers, per_layer, 1.0 / (batch_total * width), learn_rate),
        out_shape=(jax.ShapeDtypeStruct((layers, width, hidden), BF),
                   jax.ShapeDtypeStruct((layers, hidden, width), BF),
                   jax.ShapeDtypeStruct((layers, rows, width), BF),
                   jax.ShapeDtypeStruct((rows, width), F32)),
        in_specs=[any_spec] * 7,
        out_specs=(any_spec,) * 4,
        scratch_shapes=[
            pltpu.VMEM((2, 2, BLK, BLK), F32),
            pltpu.VMEM((2, 2, BLK, BLK), F32),
            pltpu.VMEM((2, 2, BLK, BLK), BF),
            pltpu.VMEM((NFULL, 2, BLK, BLK), BF),
            pltpu.VMEM((NACC, 2, HALF, BLK), BF),
            pltpu.VMEM((2, 2, HALF, BLK), BF),
            pltpu.VMEM((2, 2, HALF // 2, BLK), BF),
            pltpu.VMEM((2, 2, HALF // 4, BLK), BF),
            pltpu.VMEM((2, 2, HALF // 8, BLK), BF),
            pltpu.VMEM((2, rows, width), BF),
            pltpu.VMEM((width, rows), BF),
            pltpu.VMEM((rows, width), BF),
            pltpu.VMEM((rows, width), F32),
            pltpu.VMEM((rows, BLK), BF),
            pltpu.VMEM((2, BLK, BLK), BF),
            pltpu.VMEM((rows, width), BF),
            dma((2, 6)), dma((2,)), dma((1,)), dma((2, 2)), dma((2, 2)),
            dma((2, 2)), dma((2, 2)), dma((3, 2, 3)), dma((3, 2, 3)), dma((3, 2, 3)), dma((3, 2, 3)),
            dma((2,)), dma((2,)), dma((2, 2)),
        ],
        compiler_params=pltpu.CompilerParams(collective_id=0, has_side_effects=True, vmem_limit_bytes=66_000_000),
    )


def solution(mesh):
    n_dev = mesh.shape['pod'] * mesh.shape['data']
    rows_spec = P(('pod', 'data'), None)
    full_spec = P()

    def train_step(w_first, w_second, m_first, m_second, x_now, y_now, x_next, y_next):
        layers, model_width, _ = w_first.shape
        rows = x_now.shape[0]
        learn_rate = LEARN_BASE / layers
        kernel = build_kernel(w_first, rows, rows * n_dev, learn_rate)
        g_first, g_second, _, hidden = kernel(w_first, w_second, m_first, m_second, x_now, y_now, x_next)
        mom_first = MOMENTUM * m_first + g_first.astype(F32)
        mom_second = MOMENTUM * m_second + g_second.astype(F32)
        weight_first = w_first - learn_rate * mom_first
        weight_second = w_second - learn_rate * mom_second
        resid_rows = hidden - y_next.astype(F32)
        loss_rows = jnp.sum(resid_rows * resid_rows, axis=-1) / (2 * model_width)
        return weight_first, weight_second, mom_first, mom_second, loss_rows, hidden

    return jax.shard_map(train_step, mesh=mesh,
                         in_specs=(full_spec,) * 4 + (rows_spec,) * 4,
                         out_specs=(full_spec,) * 4 + (P(('pod', 'data')), rows_spec),
                         check_vma=False)
```

```python
import functools

import jax
import jax.numpy as jnp
from jax import lax
from jax.experimental import pallas as pl
from jax.experimental.pallas import tpu as pltpu
from jax.sharding import PartitionSpec as P

LEARN_BASE = 0.25
MOMENTUM = 0.9
GELU_C = 0.7978845608028654
GELU_A = 0.044715
BF = jnp.bfloat16
F32 = jnp.float32
MESH_ID = pl.DeviceIdType.MESH
BLK = 768
HALF = BLK // 2
PART = HALF // 3
NACC = 4
NFULL = 6
CHUNK = 256
BACK_RATE = 2
BURST_RATE = 4
NN = (((1,), (0,)), ((), ()))
NT = (((1,), (1,)), ((), ()))


def dot(lhs, rhs, dims=NN):
    return lax.dot_general(lhs, rhs, dims, preferred_element_type=F32)


def gelu(a):
    return a * (0.5 * (1.0 + jnp.tanh(GELU_C * (a + GELU_A * (a * a * a)))))


def gelu_pair(a):
    sq = a * a
    t = jnp.tanh(GELU_C * (a + GELU_A * (sq * a)))
    cdf = 0.5 * (1.0 + t)
    slope = cdf + a * (0.5 * (1.0 - t * t)) * (GELU_C * (1.0 + (3.0 * GELU_A) * sq))
    return a * cdf, slope


def step_kernel(layers, per_layer, scale, learn_rate,
                w1, w2, m1, m2, x_now, y_now, x_next,
                g1, g2, hs, h_out,
                wbuf, mbuf, gst, gfull, acc, land0, land1, land2, land3,
                hl, hl_t, low, state, actq, wlow, rows_in,
                ld_sem, hs_sem, io_sem, st_sem, own_sem,
                x0_s, x0_r, rs_s, rs_r, ag_s, ag_r, x7_s, x7_r, out_sem):
    units = layers * per_layer
    pod = lax.axis_index('pod')
    data = lax.axis_index('data')
    core = lax.rem(data, 2)
    cx = lax.rem(data // 2, 2)
    cy = data // 4
    partner = (pod, data + 1 - 2 * core)
    along = {'x': (cx, (pod, data + 2 - 4 * cx)),
             'y': (cy, (pod, data + 4 - 8 * cy)),
             'z': (pod, (1 - pod, data))}
    orders = ('xyz', 'yzx', 'zxy')

    barrier = pltpu.get_barrier_semaphore()
    for dev in (partner, along['x'][1], along['y'][1], along['z'][1]):
        pl.semaphore_signal(barrier, inc=1, device_id=dev, device_id_type=MESH_ID)
    pl.semaphore_wait(barrier, 4)

    def block_of(ref, k, layer, f):
        off = pl.multiple_of(f * BLK, BLK)
        if k == 0:
            return ref.at[layer, :, pl.ds(off, BLK)]
        return ref.at[layer, pl.ds(off, BLK), :]

    def loads(layer, f, par, full):
        out = []
        for k in range(2):
            out.append(pltpu.make_async_copy(block_of((w1, w2)[k], k, layer, f), wbuf.at[k, par], ld_sem.at[par, k]))
            if full:
                out.append(pltpu.make_async_copy(block_of((m1, m2)[k], k, layer, f), mbuf.at[k, par], ld_sem.at[par, 2 + k]))
                out.append(pltpu.make_async_copy(block_of((g1, g2)[k], k, layer, f), gst.at[k, par], ld_sem.at[par, 4 + k]))
        return out

    def start_all(copies):
        for c in copies:
            c.start()

    def wait_all(copies):
        for c in copies:
            c.wait()

    def cast_weights(par, full):
        def body(r, _):
            rows = pl.ds(pl.multiple_of(r * 64, 64), 64)
            for k in range(2):
                w = wbuf[k, par, rows, :]
                if full:
                    mom = MOMENTUM * mbuf[k, par, rows, :] + gst[k, par, rows, :].astype(F32)
                    w = w - learn_rate * mom
                wlow[k, rows, :] = w.astype(BF)
            return 0
        lax.fori_loop(0, BLK // 64, body, 0)

    def col(j):
        return pl.ds(pl.multiple_of(j * CHUNK, CHUNK), CHUNK)

    def load_rows(src):
        copy = pltpu.make_async_copy(src, rows_in, io_sem.at[0])
        copy.start()
        copy.wait()

    def save_h(layer):
        return pltpu.make_async_copy(low, hs.at[layer], hs_sem.at[0])

    def fetch_h(layer):
        slot = lax.rem(layer, 2)
        return pltpu.make_async_copy(hs.at[layer], hl.at[slot], hs_sem.at[slot])

    def forward_unit(i, full):
        layer, f, par = i // per_layer, lax.rem(i, per_layer), lax.rem(i, 2)
        wait_all(loads(layer, f, par, full))

        @pl.when(i + 1 < units)
        def _():
            nxt = i + 1
            start_all(loads(nxt // per_layer, lax.rem(nxt, per_layer), lax.rem(nxt, 2), full))

        @pl.when(f == 0)
        def _():
            if not full:
                @pl.when(layer > 0)
                def _():
                    save_h(layer - 1).wait()
            low[...] = state[...].astype(BF)
            if not full:
                save_h(layer).start()

        cast_weights(par, full)

        def first(j, _):
            a = dot(low[...], wlow[0, :, col(j)])
            actq[:, col(j)] = gelu(a).astype(BF)
            return 0
        lax.fori_loop(0, BLK // CHUNK, first, 0)

        def second(j, _):
            state[:, col(j)] += dot(actq[...], wlow[1, :, col(j)])
            return 0
        lax.fori_loop(0, BLK // CHUNK, second, 0)

    def back_place(b):
        return layers - 1 - b // per_layer, lax.rem(b, per_layer), lax.rem(b, 2)

    def store_grads(b):
        layer, f, par = back_place(b)
        return [pltpu.make_async_copy(gst.at[k, par], block_of((g1, g2)[k], k, layer, f), st_sem.at[par, k])
                for k in range(2)]

    def backward_unit(b):
        layer, f, par = back_place(b)
        wait_all(loads(layer, f, par, False))

        @pl.when(b + 1 < units)
        def _():
            nl, nf, np_ = back_place(b + 1)
            start_all(loads(nl, nf, np_, False))

        slot = lax.rem(layer, 2)

        @pl.when(f == 0)
        def _():
            fetch_h(layer).wait()

            @pl.when(layer > 0)
            def _():
                fetch_h(layer - 1).start()
            low[...] = state[...].astype(BF)
            hl_t[...] = hl[slot].T

        cast_weights(par, False)

        @pl.when(b >= 2)
        def _():
            wait_all(store_grads(b - 2))

        def body(j, _):
            a = dot(hl[slot], wlow[0, :, col(j)])
            du = dot(low[...], wlow[1, col(j), :], NT)
            u, slope = gelu_pair(a)
            q = (slope * du).astype(BF)
            actq[:, col(j)] = q
            gst[1, par, col(j), :] = dot(u.astype(BF).T, low[...]).astype(BF)
            gst[0, par, :, col(j)] = dot(hl_t[...], q).astype(BF)
            return 0
        lax.fori_loop(0, BLK // CHUNK, body, 0)

        @pl.when(layer > 0)
        def _():
            def carry(j, _):
                state[:, col(j)] += dot(actq[...], wlow[0, col(j), :], NT)
                return 0
            lax.fori_loop(0, BLK // CHUNK, carry, 0)
        start_all(store_grads(b))

    back_ticks = units // BACK_RATE
    early = back_ticks // per_layer

    def comm_place(c):
        s = c // per_layer
        layer = jnp.where(s == 0, layers - 1,
                          jnp.where(s < early, layers - 2 - s,
                                    jnp.where(s < layers - 1, s - early, layers - 2)))
        return layer, lax.rem(c, per_layer)

    def x0_copies(c):
        layer, f = comm_place(c)
        out = []
        par = lax.rem(c, 2)
        slot = lax.rem(c, NACC)
        for k in range(2):
            def rows_of(start):
                if k == 0:
                    return g1.at[layer, pl.ds(pl.multiple_of(start, HALF), HALF), pl.ds(pl.multiple_of(f * BLK, BLK), BLK)]
                return g2.at[layer, pl.ds(pl.multiple_of(f * BLK + start, HALF), HALF), :]
            out.append(pltpu.make_async_remote_copy(
                src_ref=rows_of((1 - core) * HALF), dst_ref=land0.at[par, k],
                send_sem=x0_s.at[par, k], recv_sem=x0_r.at[par, k],
                device_id=partner, device_id_type=MESH_ID))
            out.append(pltpu.make_async_copy(rows_of(core * HALF), acc.at[slot, k], own_sem.at[par, k]))
        return out

    def offsets(p):
        coords = [along[a][0] for a in orders[p]]
        keep1 = p * PART + coords[0] * (PART // 2)
        send1 = p * PART + (1 - coords[0]) * (PART // 2)
        keep2 = keep1 + coords[1] * (PART // 4)
        send2 = keep1 + (1 - coords[1]) * (PART // 4)
        keep3 = keep2 + coords[2] * (PART // 8)
        send3 = keep2 + (1 - coords[2]) * (PART // 8)
        return (keep1, keep2, keep3), (send1, send2, send3)

    places = [offsets(p) for p in range(3)]
    lands = (land1, land2, land3)
    sizes = (PART // 2, PART // 4, PART // 8)

    def rs_copies(c, j):
        par, slot = lax.rem(c, 2), lax.rem(c, NACC)
        n = sizes[j]
        return [pltpu.make_async_remote_copy(
            src_ref=acc.at[slot, :, pl.ds(pl.multiple_of(places[p][1][j], 16), n), :],
            dst_ref=lands[j].at[par, :, pl.ds(p * n, n), :],
            send_sem=rs_s.at[j, par, p], recv_sem=rs_r.at[j, par, p],
            device_id=along[orders[p][j]][1], device_id_type=MESH_ID) for p in range(3)]

    def ag_copies(c, j):
        par, slot = lax.rem(c, 2), lax.rem(c, NFULL)
        n = sizes[2 - j]
        out = []
        for p in range(3):
            rows = pl.ds(pl.multiple_of(core * HALF + places[p][0][2 - j], 16), n)
            out.append(pltpu.make_async_remote_copy(
                src_ref=gfull.at[slot, :, rows, :], dst_ref=gfull.at[slot, :, rows, :],
                send_sem=ag_s.at[j, par, p], recv_sem=ag_r.at[j, par, p],
                device_id=along[orders[p][2 - j]][1], device_id_type=MESH_ID))
        return out

    def x7_copies(c):
        par, slot = lax.rem(c, 2), lax.rem(c, NFULL)
        rows = pl.ds(pl.multiple_of(core * HALF, HALF), HALF)
        return [pltpu.make_async_remote_copy(
            src_ref=gfull.at[slot, :, rows, :], dst_ref=gfull.at[slot, :, rows, :],
            send_sem=x7_s.at[par], recv_sem=x7_r.at[par],
            device_id=partner, device_id_type=MESH_ID)]

    def out_copies(c):
        layer, f = comm_place(c)
        par, slot = lax.rem(c, 2), lax.rem(c, NFULL)
        return [pltpu.make_async_copy(gfull.at[slot, k], block_of((g1, g2)[k], k, layer, f), out_sem.at[par, k])
                for k in range(2)]

    def stage(c, s):
        @pl.when((c >= 0) & (c < units))
        def _():
            par, slot = lax.rem(c, 2), lax.rem(c, NACC)
            if s == 0:
                start_all(x0_copies(c))
            elif s == 1:
                wait_all(x0_copies(c))

                def body(r, _):
                    rows = pl.ds(pl.multiple_of(r * 64, 64), 64)
                    for k in range(2):
                        acc[slot, k, rows, :] = (acc[slot, k, rows, :].astype(F32)
                                                 + land0[par, k, rows, :].astype(F32)).astype(BF)
                    return 0
                lax.fori_loop(0, HALF // 64, body, 0)
                start_all(rs_copies(c, 0))
            elif s in (2, 3, 4):
                j = s - 2
                copies = rs_copies(c, j)
                n = sizes[j]
                full_slot = lax.rem(c, NFULL)
                for p in range(3):
                    copies[p].wait()
                    rows = pl.ds(pl.multiple_of(places[p][0][j], 16), n)
                    for k in range(2):
                        total = (acc[slot, k, rows, :].astype(F32)
                                 + lands[j][par, k, p * n:(p + 1) * n, :].astype(F32)).astype(BF)
                        if s < 4:
                            acc[slot, k, rows, :] = total
                        else:
                            own = pl.ds(pl.multiple_of(core * HALF + places[p][0][j], 16), n)
                            gfull[full_slot, k, own, :] = total
                start_all(rs_copies(c, j + 1) if s < 4 else ag_copies(c, 0))
            elif s in (5, 6):
                wait_all(ag_copies(c, s - 5))
                start_all(ag_copies(c, s - 4))
            elif s == 7:
                wait_all(ag_copies(c, 2))
                start_all(x7_copies(c))
            elif s == 8:
                wait_all(x7_copies(c))
                start_all(out_copies(c))
            else:
                wait_all(out_copies(c))

    start_all(loads(0, 0, 0, False))
    load_rows(x_now)
    state[...] = rows_in[...].astype(F32)

    def fwd_now(i, _):
        forward_unit(i, False)
        return 0
    lax.fori_loop(0, units, fwd_now, 0)
    save_h(layers - 1).wait()
    fetch_h(layers - 1).start()
    start_all(loads(layers - 1, 0, 0, False))
    load_rows(y_now)
    state[...] = (state[...] - rows_in[...].astype(F32)) * scale

    late = (layers - 1 - early) * per_layer
    first_tick = back_ticks + 11
    burst_tick = first_tick + late
    burst = (early - 1) * per_layer // BURST_RATE
    last_tick = burst_tick + burst

    def tick(t, _):
        for s in (9, 8, 7, 6, 5):
            stage(t - 1 - s, s)

        def back(j, _):
            backward_unit(BACK_RATE * t + j)
            return 0
        lax.fori_loop(0, jnp.where(t < back_ticks, BACK_RATE, 0), back, 0)

        @pl.when(t == back_ticks)
        def _():
            wait_all(store_grads(units - 2))
            wait_all(store_grads(units - 1))

        @pl.when(t == first_tick - 1)
        def _():
            start_all(loads(0, 0, 0, True))
            load_rows(x_next)
            state[...] = rows_in[...].astype(F32)

        count = jnp.where(t < first_tick, 0, jnp.where(t < burst_tick, 1, jnp.where(t < last_tick, BURST_RATE, 2 * per_layer)))
        begin = jnp.where(t < burst_tick, t - first_tick,
                          jnp.where(t < last_tick, late + BURST_RATE * (t - burst_tick), late + BURST_RATE * burst))

        def ahead(j, _):
            forward_unit(begin + j, True)
            return 0
        lax.fori_loop(0, count, ahead, 0)

        for s in (4, 3, 2, 1, 0):
            stage(t - 1 - s, s)
        return 0
    lax.fori_loop(0, last_tick + 1, tick, 0)

    copy = pltpu.make_async_copy(state, h_out, io_sem.at[0])
    copy.start()
    copy.wait()


def build_kernel(w_first, rows, batch_total, learn_rate):
    layers, width, hidden = w_first.shape
    per_layer = hidden // BLK
    any_spec = pl.BlockSpec(memory_space=pl.ANY)
    dma = pltpu.SemaphoreType.DMA
    return pl.pallas_call(
        functools.partial(step_kernel, layers, per_layer, 1.0 / (batch_total * width), learn_rate),
        out_shape=(jax.ShapeDtypeStruct((layers, width, hidden), BF),
                   jax.ShapeDtypeStruct((layers, hidden, width), BF),
                   jax.ShapeDtypeStruct((layers, rows, width), BF),
                   jax.ShapeDtypeStruct((rows, width), F32)),
        in_specs=[any_spec] * 7,
        out_specs=(any_spec,) * 4,
        scratch_shapes=[
            pltpu.VMEM((2, 2, BLK, BLK), F32),
            pltpu.VMEM((2, 2, BLK, BLK), F32),
            pltpu.VMEM((2, 2, BLK, BLK), BF),
            pltpu.VMEM((NFULL, 2, BLK, BLK), BF),
            pltpu.VMEM((NACC, 2, HALF, BLK), BF),
            pltpu.VMEM((2, 2, HALF, BLK), BF),
            pltpu.VMEM((2, 2, HALF // 2, BLK), BF),
            pltpu.VMEM((2, 2, HALF // 4, BLK), BF),
            pltpu.VMEM((2, 2, HALF // 8, BLK), BF),
            pltpu.VMEM((2, rows, width), BF),
            pltpu.VMEM((width, rows), BF),
            pltpu.VMEM((rows, width), BF),
            pltpu.VMEM((rows, width), F32),
            pltpu.VMEM((rows, BLK), BF),
            pltpu.VMEM((2, BLK, BLK), BF),
            pltpu.VMEM((rows, width), BF),
            dma((2, 6)), dma((2,)), dma((1,)), dma((2, 2)), dma((2, 2)),
            dma((2, 2)), dma((2, 2)), dma((3, 2, 3)), dma((3, 2, 3)), dma((3, 2, 3)), dma((3, 2, 3)),
            dma((2,)), dma((2,)), dma((2, 2)),
        ],
        compiler_params=pltpu.CompilerParams(collective_id=0, has_side_effects=True, vmem_limit_bytes=66_000_000),
    )


def solution(mesh):
    n_dev = mesh.shape['pod'] * mesh.shape['data']
    rows_spec = P(('pod', 'data'), None)
    full_spec = P()

    def train_step(w_first, w_second, m_first, m_second, x_now, y_now, x_next, y_next):
        layers, model_width, _ = w_first.shape
        rows = x_now.shape[0]
        learn_rate = LEARN_BASE / layers
        kernel = build_kernel(w_first, rows, rows * n_dev, learn_rate)
        g_first, g_second, _, hidden = kernel(w_first, w_second, m_first, m_second, x_now, y_now, x_next)
        mom_first = MOMENTUM * m_first + g_first.astype(F32)
        mom_second = MOMENTUM * m_second + g_second.astype(F32)
        weight_first = w_first - learn_rate * mom_first
        weight_second = w_second - learn_rate * mom_second
        resid_rows = hidden - y_next.astype(F32)
        loss_rows = jnp.sum(resid_rows * resid_rows, axis=-1) / (2 * model_width)
        return weight_first, weight_second, mom_first, mom_second, loss_rows, hidden

    return jax.shard_map(train_step, mesh=mesh,
                         in_specs=(full_spec,) * 4 + (rows_spec,) * 4,
                         out_specs=(full_spec,) * 4 + (P(('pod', 'data')), rows_spec),
                         check_vma=False)
```
